32 devices in a mesh: dp: 2 (over x), ep: 16 (over z, y, core).
Axes of the slice: x: 2, y: 2, z: 4, core: 2. Of those that a mesh axis runs over, the one named last changes fastest.
Arguments:
- hidden: bfloat16 [65536, 4096], P(('dp', 'ep')), parts along dimension 0
- ln_gamma: float32 [4096], replicated
- ln_beta: float32 [4096], replicated
- w_router: bfloat16 [4096, 16], replicated
- w_gate: bfloat16 [16, 4096, 448], P('ep')
- w_up: bfloat16 [16, 4096, 448], P('ep')
- w_down: bfloat16 [16, 448, 4096], P('ep')
- choice: int32 [65536, 2], P(('dp', 'ep')), parts along dimension 0
- mask_first: int32 [65536, 16], P(('dp', 'ep')), parts along dimension 0
- mask_second: int32 [65536, 16], P(('dp', 'ep')), parts along dimension 0
Outputs:
- output: bfloat16 [65536, 4096], P(('dp', 'ep')), parts along dimension 0
There are 2 independent parts. The reference program is written for one: setup_inputs(seed, part) draws one part's arguments, and reference() takes and returns one part's arrays. A program takes and returns all parts, laid end to end along the dimension named above; an argument that names none is the same for every part.
All inputs are finite; a program needn't handle non-finite values.
Results may differ from the reference program's by a relative error of at most 0.001.
Values are sent between devices in bfloat16 or wider.
A program may use at most 1 GiB of HBM per device.

```python
import jax
import jax.numpy as jnp
from jax import lax

D_MODEL = 4096
FF_WIDTH = 448
EXPERTS = 16
TOKENS_DEV = 2048
GROUP_DEVS = 16
TOKENS = GROUP_DEVS * TOKENS_DEV
CAPACITY = (10 * TOKENS_DEV + 4 * EXPERTS - 1) // (4 * EXPERTS)
LN_EPS = 1e-5


def draw_routing(route_key):
    sub_keys = jax.random.split(route_key, 6)
    favoured = jax.random.randint(sub_keys[0], (), 0, EXPERTS)
    coin_flip = jax.random.randint(sub_keys[1], (TOKENS,), 0, 4)
    spread = jax.random.randint(sub_keys[2], (TOKENS,), 0, EXPERTS)
    first_pick = jnp.where(coin_flip == 0, favoured, spread)
    second_pick = (first_pick + 1 + jax.random.randint(sub_keys[3], (TOKENS,), 0, EXPERTS - 1)) % EXPERTS
    expert_ids = jnp.arange(EXPERTS)
    is_first = first_pick[:, None] == expert_ids
    is_second = second_pick[:, None] == expert_ids
    keep_first = jax.random.randint(sub_keys[4], (TOKENS, EXPERTS), 0, 4) == 0
    keep_second = jax.random.randint(sub_keys[5], (TOKENS, EXPERTS), 0, 4) == 0
    mask_first = (keep_first | is_first).astype(jnp.int32)
    mask_second = ((keep_second | is_second) & (~is_first)).astype(jnp.int32)
    choice = jnp.stack([first_pick, second_pick], axis=1).astype(jnp.int32)
    return choice, mask_first, mask_second


def setup_inputs(seed: int = 0, part: int = 0) -> dict:
    shared_keys = jax.random.split(jax.random.key(seed), 6)
    part_keys = jax.random.split(jax.random.fold_in(jax.random.key(seed + 1), part), 2)
    hidden = jax.random.normal(part_keys[0], (TOKENS, D_MODEL), jnp.float32).astype(jnp.bfloat16)
    choice, mask_first, mask_second = draw_routing(part_keys[1])
    ln_gamma = 1.0 + 0.4 * jax.random.normal(shared_keys[0], (D_MODEL,), jnp.float32)
    ln_beta = 0.4 * jax.random.normal(shared_keys[1], (D_MODEL,), jnp.float32)
    w_router = (jax.random.normal(shared_keys[2], (D_MODEL, EXPERTS), jnp.float32) * D_MODEL ** -0.5).astype(jnp.bfloat16)
    w_gate = (jax.random.normal(shared_keys[3], (EXPERTS, D_MODEL, FF_WIDTH), jnp.float32) * D_MODEL ** -0.5).astype(jnp.bfloat16)
    w_up = (jax.random.normal(shared_keys[4], (EXPERTS, D_MODEL, FF_WIDTH), jnp.float32) * D_MODEL ** -0.5).astype(jnp.bfloat16)
    w_down = (jax.random.normal(shared_keys[5], (EXPERTS, FF_WIDTH, D_MODEL), jnp.float32) * FF_WIDTH ** -0.5).astype(jnp.bfloat16)
    return {"hidden": hidden, "ln_gamma": ln_gamma, "ln_beta": ln_beta, "w_router": w_router,
            "w_gate": w_gate, "w_up": w_up, "w_down": w_down, "choice": choice,
            "mask_first": mask_first, "mask_second": mask_second}


def layer_norm(token_rows, ln_gamma, ln_beta):
    values = token_rows.astype(jnp.float32)
    centred = values - jnp.mean(values, axis=-1, keepdims=True)
    variance = jnp.mean(centred * centred, axis=-1, keepdims=True)
    return (centred * lax.rsqrt(variance + LN_EPS) * ln_gamma + ln_beta).astype(jnp.bfloat16)


def reference(hidden, ln_gamma, ln_beta, w_router, w_gate, w_up, w_down, choice, mask_first, mask_second):
    normed = layer_norm(hidden, ln_gamma, ln_beta)
    scores = jnp.dot(normed, w_router, preferred_element_type=jnp.float32)
    mask_pair = jnp.stack([mask_first, mask_second], axis=1) > 0
    soft_probs = jax.nn.softmax(jnp.where(mask_pair, scores[:, None, :], -jnp.inf), axis=-1)
    gate_vals = jnp.take_along_axis(soft_probs, choice[:, :, None], axis=-1)[:, :, 0]
    by_source = choice.reshape(GROUP_DEVS, TOKENS_DEV, 2)
    expert_ids = jnp.arange(EXPERTS, dtype=jnp.int32)
    hit_count = (by_source[..., None] == expert_ids).astype(jnp.int32)
    per_token = jnp.sum(hit_count, axis=2)
    before = jnp.cumsum(per_token, axis=1) - per_token
    position = jnp.take_along_axis(before, by_source, axis=2)
    kept_copy = position < CAPACITY
    source_ids = jnp.broadcast_to(jnp.arange(GROUP_DEVS, dtype=jnp.int32)[:, None, None], by_source.shape)
    token_ids = jnp.broadcast_to(jnp.arange(TOKENS, dtype=jnp.int32).reshape(GROUP_DEVS, TOKENS_DEV, 1), by_source.shape)
    slot_table = jnp.zeros((EXPERTS, GROUP_DEVS, CAPACITY), jnp.int32)
    slot_table = slot_table.at[by_source, source_ids, position].set(token_ids, mode="drop")

    def one_expert(operands):
        row_index, gate_mat, up_mat, down_mat = operands
        expert_rows = normed[row_index.reshape(-1)]
        gate_proj = jnp.dot(expert_rows, gate_mat, preferred_element_type=jnp.float32)
        up_proj = jnp.dot(expert_rows, up_mat, preferred_element_type=jnp.float32)
        inner_act = (jax.nn.silu(gate_proj) * up_proj).astype(jnp.bfloat16)
        return jnp.dot(inner_act, down_mat, preferred_element_type=jnp.float32).astype(jnp.bfloat16)

    expert_out = lax.map(one_expert, (slot_table, w_gate, w_up, w_down))
    expert_out = expert_out.reshape(EXPERTS, GROUP_DEVS, CAPACITY, D_MODEL)
    picked = expert_out[by_source, source_ids, jnp.minimum(position, CAPACITY - 1)]
    kept_gates = jnp.where(kept_copy, gate_vals.reshape(GROUP_DEVS, TOKENS_DEV, 2), 0.0)
    mixed_out = hidden.reshape(GROUP_DEVS, TOKENS_DEV, D_MODEL).astype(jnp.float32) + jnp.sum(kept_gates[..., None] * picked.astype(jnp.float32), axis=2)
    return mixed_out.reshape(TOKENS, D_MODEL).astype(jnp.bfloat16)
```

```python
import jax
import jax.numpy as jnp
from jax import lax
from jax.sharding import PartitionSpec as P

LN_EPS = 1e-5


def layer_norm(token_rows, ln_gamma, ln_beta):
    values = token_rows.astype(jnp.float32)
    centred = values - jnp.mean(values, axis=-1, keepdims=True)
    variance = jnp.mean(centred * centred, axis=-1, keepdims=True)
    return (centred * lax.rsqrt(variance + LN_EPS) * ln_gamma + ln_beta).astype(jnp.bfloat16)


def sparse_gates(normed, w_router, choice, mask_first, mask_second):
    scores = jnp.dot(normed, w_router, preferred_element_type=jnp.float32)
    expert_ids = jnp.arange(w_router.shape[1], dtype=jnp.int32)
    gates = []
    for j, mask in enumerate((mask_first, mask_second)):
        probs = jax.nn.softmax(jnp.where(mask > 0, scores, -jnp.inf), axis=-1)
        gates.append(jnp.sum(jnp.where(choice[:, j:j + 1] == expert_ids, probs, 0.0), axis=-1))
    return gates


def copy_slots(choice, experts):
    expert_ids = jnp.arange(experts, dtype=jnp.int32)
    hit_count = (choice[..., None] == expert_ids).astype(jnp.int32)
    per_token = jnp.sum(hit_count, axis=-2)
    before = jnp.cumsum(per_token, axis=-2) - per_token
    return jnp.sum(hit_count * before[..., None, :], axis=-1)


def solution(mesh):
    group_size = mesh.shape["ep"]
    rows_spec = P(("dp", "ep"))
    core_groups = [list(range(core, group_size, 2)) for core in range(2)]
    partner_pairs = [(k, k ^ 1) for k in range(group_size)]

    def device_step(hidden, ln_gamma, ln_beta, w_router, w_gate, w_up, w_down, choice, mask_first, mask_second):
        tokens, row_width = hidden.shape
        chips = group_size // 2
        experts = group_size
        ff_width = w_gate.shape[2]
        capacity = (10 * tokens + 4 * experts - 1) // (4 * experts)
        half_slots = chips * capacity
        side = lax.axis_index("dp")
        core = lax.rem(lax.axis_index("ep"), 2)
        on_left = side == 0

        ff_half = 128
        ff_split = 2 * ff_half
        col_half = 1024
        col_split = 2 * col_half
        col_rest = [(col_split + i * 1024, 1024) for i in range(2)]

        gate_rows, up_rows, down_rows = w_gate[0].T, w_up[0].T, w_down[0]

        def gather(piece):
            return lax.all_gather(piece[None], "ep", axis=0, tiled=True, axis_index_groups=core_groups)

        def swap(piece):
            return lax.ppermute(piece, "dp", [(0, 1), (1, 0)])

        gate_own = gather(lax.dynamic_slice_in_dim(gate_rows, side * ff_half, ff_half, 0))
        gate_far = swap(gate_own)
        up_own = gather(lax.dynamic_slice_in_dim(up_rows, side * ff_half, ff_half, 0))
        up_far = swap(up_own)
        down_own = gather(lax.dynamic_slice_in_dim(down_rows, side * col_half, col_half, 1))
        down_far = swap(down_own)
        gate_rest = gather(gate_rows[ff_split:])
        up_rest = gather(up_rows[ff_split:])
        down_rest = [gather(down_rows[:, start:start + width]) for start, width in col_rest]

        normed = layer_norm(hidden, ln_gamma, ln_beta)
        position = copy_slots(choice, experts)
        slot = jnp.where(lax.rem(choice, 2) == core, 0, half_slots) + (choice // 2) * capacity
        flat_slot = jnp.where(position < capacity, slot + position, 2 * half_slots)
        token_ids = jnp.broadcast_to(jnp.arange(tokens, dtype=jnp.int32)[:, None], (tokens, 2))
        source_row = jnp.zeros((2 * half_slots,), jnp.int32).at[flat_slot.reshape(-1)].set(token_ids.reshape(-1), mode="drop")
        away_rows = jnp.take(normed, source_row[half_slots:], axis=0, mode="clip").reshape(chips, capacity, row_width)
        guest_rows = lax.ppermute(away_rows, "ep", partner_pairs)
        home_rows = jnp.take(normed, source_row[:half_slots], axis=0, mode="clip").reshape(chips, capacity, row_width)
        rows = jnp.concatenate([home_rows, guest_rows], axis=1)

        gates = sparse_gates(normed, w_router, choice, mask_first, mask_second)
        gates = [jnp.where(position[:, j] < capacity, gates[j], 0.0)[:, None] for j in range(2)]
        pick_slot = slot + jnp.minimum(position, capacity - 1)

        def inner(gate_w, up_w):
            gate_proj = jnp.einsum("erd,efd->erf", rows, gate_w, preferred_element_type=jnp.float32)
            up_proj = jnp.einsum("erd,efd->erf", rows, up_w, preferred_element_type=jnp.float32)
            return (jax.nn.silu(gate_proj) * up_proj).astype(jnp.bfloat16)

        act_own = inner(gate_own, up_own)
        act_far = inner(gate_far, up_far)
        act_rest = inner(gate_rest, up_rest)
        act = jnp.concatenate([jnp.where(on_left, act_own, act_far), jnp.where(on_left, act_far, act_own), act_rest], axis=2)

        def mixed(down_w):
            width = down_w.shape[2]
            out_rows = jnp.einsum("erf,efd->erd", act, down_w, preferred_element_type=jnp.float32).astype(jnp.bfloat16)
            back = lax.ppermute(out_rows[:, capacity:], "ep", partner_pairs)
            table = jnp.concatenate([out_rows[:, :capacity], back], axis=0).reshape(2 * half_slots, width)
            first, second = [jnp.take(table, pick_slot[:, j], axis=0, mode="clip").astype(jnp.float32) for j in range(2)]
            return gates[0] * first + gates[1] * second

        mix_own, mix_far = mixed(down_own), mixed(down_far)
        blocks = [jnp.where(on_left, mix_own, mix_far), jnp.where(on_left, mix_far, mix_own)] + [mixed(w) for w in down_rest]
        starts = [0, col_half] + [start for start, _ in col_rest]
        outs = [(hidden[:, start:start + block.shape[1]].astype(jnp.float32) + block).astype(jnp.bfloat16)
                for start, block in zip(starts, blocks)]
        return jnp.concatenate(outs, axis=1)

    return jax.shard_map(device_step, mesh=mesh,
                         in_specs=(rows_spec, P(), P(), P(), P("ep"), P("ep"), P("ep"), rows_spec, rows_spec, rows_spec),
                         out_specs=rows_spec, check_vma=False)
```

```python
import functools

import jax
import jax.numpy as jnp
from jax import lax
from jax.experimental import pallas as pl
from jax.experimental.pallas import tpu as pltpu
from jax.sharding import PartitionSpec as P

LN_EPS = 1e-5


def layer_norm(token_rows, ln_gamma, ln_beta):
    values = token_rows.astype(jnp.float32)
    centred = values - jnp.mean(values, axis=-1, keepdims=True)
    variance = jnp.mean(centred * centred, axis=-1, keepdims=True)
    return (centred * lax.rsqrt(variance + LN_EPS) * ln_gamma + ln_beta).astype(jnp.bfloat16)


def sparse_gates(normed, w_router, choice, mask_first, mask_second):
    scores = jnp.dot(normed, w_router, preferred_element_type=jnp.float32)
    expert_ids = jnp.arange(w_router.shape[1], dtype=jnp.int32)
    gates = []
    for j, mask in enumerate((mask_first, mask_second)):
        probs = jax.nn.softmax(jnp.where(mask > 0, scores, -jnp.inf), axis=-1)
        gates.append(jnp.sum(jnp.where(choice[:, j:j + 1] == expert_ids, probs, 0.0), axis=-1))
    return gates


def copy_slots(choice, experts):
    expert_ids = jnp.arange(experts, dtype=jnp.int32)
    hit_count = (choice[..., None] == expert_ids).astype(jnp.int32)
    per_token = jnp.sum(hit_count, axis=-2)
    before = jnp.cumsum(per_token, axis=-2) - per_token
    return jnp.sum(hit_count * before[..., None, :], axis=-1)


def mix_kernel(width, weight_col, has_prev, n_weights, where, pick_a, pick_b, gate_a, gate_b, act, hidden, *refs):
    weights, refs = refs[:n_weights], refs[n_weights + (1 if has_prev else 0):]
    out, table, mix, x_buf, o_buf, w_buf, w_sem, x_sem, o_sem = refs
    _, capacity, _ = act.shape
    tokens = x_buf.shape[0]
    tiles = width // 128
    step = min(256, width)
    block = mix.shape[0]
    col = pl.multiple_of(where[0], 128)
    load_x = pltpu.make_async_copy(hidden.at[:, pl.ds(col, width)], x_buf, x_sem)
    load_x.start()

    def load_w(source, i, slot):
        return pltpu.make_async_copy(source.at[i, :, pl.ds(weight_col, width)], w_buf.at[slot], w_sem.at[slot])

    for k, source in enumerate(weights):
        count = source.shape[0]
        load_w(source, 0, 0).start()

        @pl.loop(0, count)
        def _(i):
            slot = lax.rem(i, 2)

            @pl.when(i + 1 < count)
            def _():
                load_w(source, i + 1, 1 - slot).start()

            load_w(source, i, slot).wait()
            if n_weights == 1:
                expert = i
            else:
                expert = 2 * i + (where[1] if k == 0 else 1 - where[1])
            rows = pl.ds(pl.multiple_of(expert * capacity, 8), capacity)
            lhs = act[expert]
            for start in range(0, width, step):
                prod = jnp.dot(lhs, w_buf[slot, :, start:start + step], preferred_element_type=jnp.float32)
                prod = prod.astype(jnp.bfloat16).astype(jnp.float32)
                for j in range(step // 128):
                    table[rows, start // 128 + j, :] = prod[:, j * 128:(j + 1) * 128]

    load_x.wait()

    @pl.loop(0, tokens // block)
    def _(b):
        base = pl.multiple_of(b * block, block)

        @pl.loop(0, block // 8)
        def _(i):
            for k in range(8):
                t = base + i * 8 + k
                mix[i * 8 + k] = gate_a[t] * table[pick_a[t]] + gate_b[t] * table[pick_b[t]]

        for j in range(tiles):
            cols = slice(j * 128, (j + 1) * 128)
            total = x_buf[pl.ds(base, block), cols].astype(jnp.float32) + mix[:, j, :]
            o_buf[pl.ds(base, block), cols] = total.astype(jnp.bfloat16)

    store = pltpu.make_async_copy(o_buf, out.at[:, pl.ds(col, width)], o_sem)
    store.start()
    store.wait()


def mix_columns(where, picks, gates, act, hidden, weights, prev, width, weight_col=0):
    experts, capacity, ff_width = act.shape
    tokens = hidden.shape[0]
    tiles = width // 128
    has_prev = prev is not None
    smem, vmem, hbm = [pl.BlockSpec(memory_space=space) for space in (pltpu.SMEM, pltpu.VMEM, pl.ANY)]
    operands = [where, *picks, *gates, act, hidden, *weights] + ([prev] if has_prev else [])
    return pl.pallas_call(
        functools.partial(mix_kernel, width, weight_col, has_prev, len(weights)),
        out_shape=jax.ShapeDtypeStruct(hidden.shape, hidden.dtype),
        in_specs=[smem] * 5 + [vmem] + [hbm] * (len(operands) - 6),
        out_specs=hbm,
        scratch_shapes=[
            pltpu.VMEM((experts * capacity, tiles, 128), jnp.float32),
            pltpu.VMEM((128, tiles, 128), jnp.float32),
            pltpu.VMEM((tokens, width), jnp.bfloat16),
            pltpu.VMEM((tokens, width), jnp.bfloat16),
            pltpu.VMEM((2, ff_width, width), jnp.bfloat16),
            pltpu.SemaphoreType.DMA((2,)),
            pltpu.SemaphoreType.DMA,
            pltpu.SemaphoreType.DMA,
        ],
        input_output_aliases={len(operands) - 1: 0} if has_prev else {},
        cost_estimate=pl.CostEstimate(flops=2 * experts * capacity * ff_width * width,
                                      bytes_accessed=2 * (experts * ff_width * (width + capacity) + 2 * tokens * width),
                                      transcendentals=0),
        compiler_params=pltpu.CompilerParams(vmem_limit_bytes=56 * 1024 * 1024),
    )(*operands)


def solution(mesh):
    group_size = mesh.shape["ep"]
    rows_spec = P(("dp", "ep"))
    partner_pairs = [(k, k ^ 1) for k in range(group_size)]

    def device_step(hidden, ln_gamma, ln_beta, w_router, w_gate, w_up, w_down, choice, mask_first, mask_second):
        tokens, row_width = hidden.shape
        experts = group_size
        chips = group_size // 2
        capacity = (10 * tokens + 4 * experts - 1) // (4 * experts)
        slot_count = experts * capacity
        side = lax.axis_index("dp")
        core = lax.rem(lax.axis_index("ep"), 2)
        on_left, first_core = side == 0, core == 0

        ff_half, col_half = 112, 1280
        ff_split, col_split = 2 * ff_half, 2 * col_half
        wide = 1024

        gate_rows, up_rows, down_rows = w_gate[0].T, w_up[0].T, w_down[0]

        def gather(piece):
            return lax.all_gather(piece[None], "ep", axis=0, tiled=True)

        def swap(mine):
            far = lax.ppermute(mine, "dp", [(0, 1), (1, 0)])
            return far, lax.ppermute(far, "ep", partner_pairs)

        def same_core(own):
            return lax.dynamic_index_in_dim(own.reshape(chips, 2, *own.shape[1:]), core, 1, keepdims=False)

        half_rows = [lax.dynamic_slice_in_dim(w, side * ff_half, ff_half, 0) for w in (gate_rows, up_rows)]
        gu_own = gather(jnp.concatenate(half_rows, axis=0))
        down_own = gather(lax.dynamic_slice_in_dim(down_rows, side * col_half, col_half, 1))
        gate_rest = gather(gate_rows[ff_split:])
        up_rest = gather(up_rows[ff_split:])
        cut_rest = down_rows[:, col_split:]
        down_rest = gather(cut_rest)

        gu_mine = same_core(gu_own)
        gu_far, gu_other = swap(gu_mine)
        even, odd = jnp.where(first_core, gu_far, gu_other), jnp.where(first_core, gu_other, gu_far)
        gu_far = jnp.concatenate([even, odd], axis=1).reshape(gu_own.shape)
        down_mine = same_core(down_own)
        down_wide, down_slim = down_mine[:, :, :wide], down_mine[:, :, wide:]
        down_wide = swap(down_wide)
        down_slim = swap(down_slim)

        normed = layer_norm(hidden, ln_gamma, ln_beta)
        position = copy_slots(choice, experts)
        flat_slot = jnp.where(position < capacity, choice * capacity + position, slot_count)
        token_ids = jnp.broadcast_to(jnp.arange(tokens, dtype=jnp.int32)[:, None], (tokens, 2))
        source_row = jnp.zeros((slot_count,), jnp.int32).at[flat_slot.reshape(-1)].set(token_ids.reshape(-1), mode="drop")
        rows = jnp.take(normed, source_row, axis=0, mode="clip").reshape(experts, capacity, row_width)

        gates = sparse_gates(normed, w_router, choice, mask_first, mask_second)
        gates = [jnp.where(position[:, j] < capacity, gates[j], 0.0) for j in range(2)]
        pick_slot = choice * capacity + jnp.minimum(position, capacity - 1)
        picks = [pick_slot[:, j] for j in range(2)]
        rows, gates, picks = lax.optimization_barrier((rows, gates, picks))

        def project(weight):
            return jnp.einsum("erd,efd->erf", rows, weight, preferred_element_type=jnp.float32)

        def activate(gate_proj, up_proj):
            return (jax.nn.silu(gate_proj) * up_proj).astype(jnp.bfloat16)

        both = project(gu_own)
        act_own = activate(both[:, :, :ff_half], both[:, :, ff_half:])
        both = project(gu_far)
        act_far = activate(both[:, :, :ff_half], both[:, :, ff_half:])
        act_rest = activate(project(gate_rest), project(up_rest))
        act = jnp.concatenate([jnp.where(on_left, act_own, act_far), jnp.where(on_left, act_far, act_own), act_rest], axis=2)

        def place(prev, weights, start, width, weight_col=0):
            where = jnp.stack([jnp.asarray(start, jnp.int32), core.astype(jnp.int32)])
            return mix_columns(where, picks, gates, act, hidden, weights, prev, width, weight_col)

        own_start, far_start = side * col_half, (1 - side) * col_half
        slim, rest = col_half - wide, row_width - col_split - wide
        out = place(None, (down_own,), own_start, wide)
        out = place(out, (down_own,), own_start + wide, slim, wide)
        out = place(out, down_wide, far_start, wide)
        out = place(out, (down_rest,), col_split, wide)
        out = place(out, (down_rest,), col_split + wide, rest, wide)
        return place(out, down_slim, far_start + wide, slim)

    return jax.shard_map(device_step, mesh=mesh,
                         in_specs=(rows_spec, P(), P(), P(), P("ep"), P("ep"), P("ep"), rows_spec, rows_spec, rows_spec),
                         out_specs=rows_spec, check_vma=False)
```

```python
import functools

import jax
import jax.numpy as jnp
from jax import lax
from jax.experimental import pallas as pl
from jax.experimental.pallas import tpu as pltpu
from jax.sharding import PartitionSpec as P

LN_EPS = 1e-5


def layer_norm(token_rows, ln_gamma, ln_beta):
    values = token_rows.astype(jnp.float32)
    centred = values - jnp.mean(values, axis=-1, keepdims=True)
    variance = jnp.mean(centred * centred, axis=-1, keepdims=True)
    return (centred * lax.rsqrt(variance + LN_EPS) * ln_gamma + ln_beta).astype(jnp.bfloat16)


def sparse_gates(normed, w_router, choice, mask_first, mask_second):
    scores = jnp.dot(normed, w_router, preferred_element_type=jnp.float32)
    expert_ids = jnp.arange(w_router.shape[1], dtype=jnp.int32)
    gates = []
    for j, mask in enumerate((mask_first, mask_second)):
        probs = jax.nn.softmax(jnp.where(mask > 0, scores, -jnp.inf), axis=-1)
        gates.append(jnp.sum(jnp.where(choice[:, j:j + 1] == expert_ids, probs, 0.0), axis=-1))
    return gates


def copy_slots(choice, experts):
    expert_ids = jnp.arange(experts, dtype=jnp.int32)
    hit_count = (choice[..., None] == expert_ids).astype(jnp.int32)
    per_token = jnp.sum(hit_count, axis=-2)
    before = jnp.cumsum(per_token, axis=-2) - per_token
    return jnp.sum(hit_count * before[..., None, :], axis=-1)


def mix_kernel(width, weight_col, has_prev, n_weights, where, pick_a, pick_b, gate_a, gate_b, act, hidden, *refs):
    weights, refs = refs[:n_weights], refs[n_weights + (1 if has_prev else 0):]
    out, table, mix, x_buf, o_buf, w_buf, w_sem, x_sem, o_sem = refs
    _, capacity, _ = act.shape
    tokens = x_buf.shape[0]
    tiles = width // 128
    step = min(256, width)
    block = mix.shape[0]
    col = pl.multiple_of(where[0], 128)
    load_x = pltpu.make_async_copy(hidden.at[:, pl.ds(col, width)], x_buf, x_sem)
    load_x.start()

    def load_w(source, i, slot):
        return pltpu.make_async_copy(source.at[i, :, pl.ds(weight_col, width)], w_buf.at[slot], w_sem.at[slot])

    for k, source in enumerate(weights):
        count = source.shape[0]
        load_w(source, 0, 0).start()

        @pl.loop(0, count)
        def _(i):
            slot = lax.rem(i, 2)

            @pl.when(i + 1 < count)
            def _():
                load_w(source, i + 1, 1 - slot).start()

            load_w(source, i, slot).wait()
            if n_weights == 1:
                expert = i
            else:
                expert = 2 * i + (where[1] if k == 0 else 1 - where[1])
            rows = pl.ds(pl.multiple_of(expert * capacity, 8), capacity)
            lhs = act[expert]
            for start in range(0, width, step):
                prod = jnp.dot(lhs, w_buf[slot, :, start:start + step], preferred_element_type=jnp.float32)
                prod = prod.astype(jnp.bfloat16).astype(jnp.float32)
                for j in range(step // 128):
                    table[rows, start // 128 + j, :] = prod[:, j * 128:(j + 1) * 128]

    load_x.wait()

    @pl.loop(0, tokens // block)
    def _(b):
        base = pl.multiple_of(b * block, block)

        @pl.loop(0, block // 16)
        def _(i):
            slots = [base + i * 16 + k for k in range(16)]
            picked = [(table[pick_a[t]], table[pick_b[t]]) for t in slots]
            sums = [gate_a[t] * first + gate_b[t] * second for t, (first, second) in zip(slots, picked)]
            for k in range(16):
                mix[i * 16 + k] = sums[k]

        for j in range(tiles):
            cols = slice(j * 128, (j + 1) * 128)
            total = x_buf[pl.ds(base, block), cols].astype(jnp.float32) + mix[:, j, :]
            o_buf[pl.ds(base, block), cols] = total.astype(jnp.bfloat16)

    store = pltpu.make_async_copy(o_buf, out.at[:, pl.ds(col, width)], o_sem)
    store.start()
    store.wait()


def mix_columns(where, picks, gates, act, hidden, weights, prev, width, weight_col=0):
    experts, capacity, ff_width = act.shape
    tokens = hidden.shape[0]
    tiles = width // 128
    has_prev = prev is not None
    smem, vmem, hbm = [pl.BlockSpec(memory_space=space) for space in (pltpu.SMEM, pltpu.VMEM, pl.ANY)]
    operands = [where, *picks, *gates, act, hidden, *weights] + ([prev] if has_prev else [])
    return pl.pallas_call(
        functools.partial(mix_kernel, width, weight_col, has_prev, len(weights)),
        out_shape=jax.ShapeDtypeStruct(hidden.shape, hidden.dtype),
        in_specs=[smem] * 5 + [vmem] + [hbm] * (len(operands) - 6),
        out_specs=hbm,
        scratch_shapes=[
            pltpu.VMEM((experts * capacity, tiles, 128), jnp.float32),
            pltpu.VMEM((128, tiles, 128), jnp.float32),
            pltpu.VMEM((tokens, width), jnp.bfloat16),
            pltpu.VMEM((tokens, width), jnp.bfloat16),
            pltpu.VMEM((2, ff_width, width), jnp.bfloat16),
            pltpu.SemaphoreType.DMA((2,)),
            pltpu.SemaphoreType.DMA,
            pltpu.SemaphoreType.DMA,
        ],
        input_output_aliases={len(operands) - 1: 0} if has_prev else {},
        cost_estimate=pl.CostEstimate(flops=2 * experts * capacity * ff_width * width,
                                      bytes_accessed=2 * (experts * ff_width * (width + capacity) + 2 * tokens * width),
                                      transcendentals=0),
        compiler_params=pltpu.CompilerParams(vmem_limit_bytes=56 * 1024 * 1024),
    )(*operands)


def solution(mesh):
    group_size = mesh.shape["ep"]
    rows_spec = P(("dp", "ep"))
    partner_pairs = [(k, k ^ 1) for k in range(group_size)]

    def device_step(hidden, ln_gamma, ln_beta, w_router, w_gate, w_up, w_down, choice, mask_first, mask_second):
        tokens, row_width = hidden.shape
        experts = group_size
        chips = group_size // 2
        capacity = (10 * tokens + 4 * experts - 1) // (4 * experts)
        slot_count = experts * capacity
        side = lax.axis_index("dp")
        core = lax.rem(lax.axis_index("ep"), 2)
        on_left, first_core = side == 0, core == 0

        ff_half, col_half = 112, 1280
        ff_split, col_split = 2 * ff_half, 2 * col_half
        wide = 1024

        gate_rows, up_rows, down_rows = w_gate[0].T, w_up[0].T, w_down[0]

        def gather(piece):
            return lax.all_gather(piece[None], "ep", axis=0, tiled=True)

        def swap(mine):
            far = lax.ppermute(mine, "dp", [(0, 1), (1, 0)])
            return far, lax.ppermute(far, "ep", partner_pairs)

        def same_core(own):
            return lax.dynamic_index_in_dim(own.reshape(chips, 2, *own.shape[1:]), core, 1, keepdims=False)

        half_rows = [lax.dynamic_slice_in_dim(w, side * ff_half, ff_half, 0) for w in (gate_rows, up_rows)]
        gu_own = gather(jnp.concatenate(half_rows, axis=0))
        down_own = gather(lax.dynamic_slice_in_dim(down_rows, side * col_half, col_half, 1))
        gate_rest = gather(gate_rows[ff_split:])
        up_rest = gather(up_rows[ff_split:])
        cut_rest = down_rows[:, col_split:]
        down_rest = gather(cut_rest)

        gu_mine = same_core(gu_own)
        gu_far, gu_other = swap(gu_mine)
        down_mine = same_core(down_own)
        down_wide, down_slim = down_mine[:, :, :wide], down_mine[:, :, wide:]
        down_wide = swap(down_wide)
        down_slim = swap(down_slim)

        normed = layer_norm(hidden, ln_gamma, ln_beta)
        position = copy_slots(choice, experts)
        flat_slot = jnp.where(position < capacity, choice * capacity + position, slot_count)
        token_ids = jnp.broadcast_to(jnp.arange(tokens, dtype=jnp.int32)[:, None], (tokens, 2))
        source_row = jnp.zeros((slot_count,), jnp.int32).at[flat_slot.reshape(-1)].set(token_ids.reshape(-1), mode="drop")
        rows = jnp.take(normed, source_row, axis=0, mode="clip").reshape(experts, capacity, row_width)

        gates = sparse_gates(normed, w_router, choice, mask_first, mask_second)
        gates = [jnp.where(position[:, j] < capacity, gates[j], 0.0) for j in range(2)]
        pick_slot = choice * capacity + jnp.minimum(position, capacity - 1)
        picks = [pick_slot[:, j] for j in range(2)]
        rows, gates, picks = lax.optimization_barrier((rows, gates, picks))

        by_core = rows.reshape(chips, 2, capacity, row_width)
        rows_mine = lax.dynamic_index_in_dim(by_core, core, 1, keepdims=False)
        rows_other = lax.dynamic_index_in_dim(by_core, 1 - core, 1, keepdims=False)

        def project(weight, rows=rows):
            return jnp.einsum("erd,efd->erf", rows, weight, preferred_element_type=jnp.float32)

        def activate(gate_proj, up_proj):
            return (jax.nn.silu(gate_proj) * up_proj).astype(jnp.bfloat16)

        def activate_both(both):
            return activate(both[:, :, :ff_half], both[:, :, ff_half:])

        act_own = activate_both(project(gu_own))
        act_mine = activate_both(project(gu_far, rows_mine))
        act_other = activate_both(project(gu_other, rows_other))
        even, odd = jnp.where(first_core, act_mine, act_other), jnp.where(first_core, act_other, act_mine)
        act_far = jnp.concatenate([even, odd], axis=1).reshape(act_own.shape)
        act_rest = activate(project(gate_rest), project(up_rest))
        act = jnp.concatenate([jnp.where(on_left, act_own, act_far), jnp.where(on_left, act_far, act_own), act_rest], axis=2)

        def place(prev, weights, start, width, weight_col=0):
            where = jnp.stack([jnp.asarray(start, jnp.int32), core.astype(jnp.int32)])
            return mix_columns(where, picks, gates, act, hidden, weights, prev, width, weight_col)

        own_start, far_start = side * col_half, (1 - side) * col_half
        slim, rest = col_half - wide, row_width - col_split - wide
        out = place(None, (down_own,), own_start, wide)
        out = place(out, (down_own,), own_start + wide, slim, wide)
        out = place(out, down_wide, far_start, wide)
        out = place(out, (down_rest,), col_split, wide)
        out = place(out, (down_rest,), col_split + wide, rest, wide)
        return place(out, down_slim, far_start + wide, slim)

    return jax.shard_map(device_step, mesh=mesh,
                         in_specs=(rows_spec, P(), P(), P(), P("ep"), P("ep"), P("ep"), rows_spec, rows_spec, rows_spec),
                         out_specs=rows_spec, check_vma=False)
```

```python
import functools

import jax
import jax.numpy as jnp
from jax import lax
from jax.experimental import pallas as pl
from jax.experimental.pallas import tpu as pltpu
from jax.sharding import PartitionSpec as P

LN_EPS = 1e-5


def layer_norm(token_rows, ln_gamma, ln_beta):
    values = token_rows.astype(jnp.float32)
    centred = values - jnp.mean(values, axis=-1, keepdims=True)
    variance = jnp.mean(centred * centred, axis=-1, keepdims=True)
    return (centred * lax.rsqrt(variance + LN_EPS) * ln_gamma + ln_beta).astype(jnp.bfloat16)


def sparse_gates(normed, w_router, choice, mask_first, mask_second):
    scores = jnp.dot(normed, w_router, preferred_element_type=jnp.float32)
    expert_ids = jnp.arange(w_router.shape[1], dtype=jnp.int32)
    gates = []
    for j, mask in enumerate((mask_first, mask_second)):
        probs = jax.nn.softmax(jnp.where(mask > 0, scores, -jnp.inf), axis=-1)
        gates.append(jnp.sum(jnp.where(choice[:, j:j + 1] == expert_ids, probs, 0.0), axis=-1))
    return gates


def copy_slots(choice, experts):
    expert_ids = jnp.arange(experts, dtype=jnp.int32)
    hit_count = (choice[..., None] == expert_ids).astype(jnp.int32)
    per_token = jnp.sum(hit_count, axis=-2)
    before = jnp.cumsum(per_token, axis=-2) - per_token
    return jnp.sum(hit_count * before[..., None, :], axis=-1)


def mix_kernel(width, weight_col, has_prev, n_weights, where, pick_a, pick_b, gate_a, gate_b, act, hidden, *refs):
    weights, refs = refs[:n_weights], refs[n_weights + (1 if has_prev else 0):]
    out, table, mix, x_buf, o_buf, w_buf, w_sem, x_sem, o_sem = refs
    capacity = act.shape[1]
    tokens = x_buf.shape[0]
    step = min(256, width)
    block = mix.shape[0] // 8
    col = pl.multiple_of(where[0], 128)

    def load_w(source, first, i):
        return pltpu.make_async_copy(source.at[i, :, pl.ds(weight_col, width)], w_buf.at[first + i], w_sem.at[first + i])

    firsts = [sum(source.shape[0] for source in weights[:k]) for k in range(n_weights)]
    for source, first in zip(weights, firsts):
        for i in range(source.shape[0]):
            load_w(source, first, i).start()
    load_x = pltpu.make_async_copy(hidden.at[:, pl.ds(col, width)], x_buf, x_sem)
    load_x.start()

    for k, (source, first) in enumerate(zip(weights, firsts)):
        @pl.loop(0, source.shape[0])
        def _(i):
            load_w(source, first, i).wait()
            if n_weights == 1:
                expert = i
            else:
                expert = 2 * i + (where[1] if k == 0 else 1 - where[1])
            base = pl.multiple_of(expert * (capacity * 8), 8)
            lhs = act[expert]
            for start in range(0, width, step):
                prod = jnp.dot(lhs, w_buf[first + i, :, start:start + step], preferred_element_type=jnp.float32)
                prod = prod.astype(jnp.bfloat16).astype(jnp.float32)
                for j in range(step // 128):
                    table[pl.ds(base + start // 128 + j, capacity, stride=8), :] = prod[:, j * 128:(j + 1) * 128]

    load_x.wait()

    def row_of(pick):
        return table[pl.ds(pl.multiple_of(pick * 8, 8), 8), :]

    @pl.loop(0, tokens // block)
    def _(b):
        base = pl.multiple_of(b * block, block)

        @pl.loop(0, block // 16)
        def _(i):
            slots = [base + i * 16 + k for k in range(16)]
            picked = [(row_of(pick_a[t]), row_of(pick_b[t])) for t in slots]
            sums = [gate_a[t] * first + gate_b[t] * second for t, (first, second) in zip(slots, picked)]
            for k in range(16):
                mix[pl.ds(pl.multiple_of(i * 128 + k * 8, 8), 8), :] = sums[k]

        for j in range(width // 128):
            cols = slice(j * 128, (j + 1) * 128)
            total = x_buf[pl.ds(base, block), cols].astype(jnp.float32) + mix[pl.ds(j, block, stride=8), :]
            o_buf[pl.ds(base, block), cols] = total.astype(jnp.bfloat16)

    store = pltpu.make_async_copy(o_buf, out.at[:, pl.ds(col, width)], o_sem)
    store.start()
    store.wait()


def mix_columns(where, picks, gates, act, hidden, weights, prev, width, weight_col=0):
    experts, capacity, ff_width = act.shape
    tokens = hidden.shape[0]
    has_prev = prev is not None
    smem, vmem, hbm = [pl.BlockSpec(memory_space=space) for space in (pltpu.SMEM, pltpu.VMEM, pl.ANY)]
    operands = [where, *picks, *gates, act, hidden, *weights] + ([prev] if has_prev else [])
    return pl.pallas_call(
        functools.partial(mix_kernel, width, weight_col, has_prev, len(weights)),
        out_shape=jax.ShapeDtypeStruct(hidden.shape, hidden.dtype),
        in_specs=[smem] * 5 + [vmem] + [hbm] * (len(operands) - 6),
        out_specs=hbm,
        scratch_shapes=[
            pltpu.VMEM((experts * capacity * 8, 128), jnp.float32),
            pltpu.VMEM((128 * 8, 128), jnp.float32),
            pltpu.VMEM((tokens, width), jnp.bfloat16),
            pltpu.VMEM((tokens, width), jnp.bfloat16),
            pltpu.VMEM((experts, ff_width, width), jnp.bfloat16),
            pltpu.SemaphoreType.DMA((experts,)),
            pltpu.SemaphoreType.DMA,
            pltpu.SemaphoreType.DMA,
        ],
        input_output_aliases={len(operands) - 1: 0} if has_prev else {},
        cost_estimate=pl.CostEstimate(flops=2 * experts * capacity * ff_width * width,
                                      bytes_accessed=2 * (experts * ff_width * (width + capacity) + 2 * tokens * width),
                                      transcendentals=0),
        compiler_params=pltpu.CompilerParams(vmem_limit_bytes=56 * 1024 * 1024),
    )(*operands)


def solution(mesh):
    group_size = mesh.shape["ep"]
    rows_spec = P(("dp", "ep"))
    partner_pairs = [(k, k ^ 1) for k in range(group_size)]

    def device_step(hidden, ln_gamma, ln_beta, w_router, w_gate, w_up, w_down, choice, mask_first, mask_second):
        tokens, row_width = hidden.shape
        experts = group_size
        chips = group_size // 2
        capacity = (10 * tokens + 4 * experts - 1) // (4 * experts)
        slot_count = experts * capacity
        side = lax.axis_index("dp")
        core = lax.rem(lax.axis_index("ep"), 2)
        on_left, first_core = side == 0, core == 0

        ff_half, col_half = 104, 1280
        ff_split, col_split = 2 * ff_half, 2 * col_half
        wide = 1024

        gate_rows, up_rows, down_rows = w_gate[0].T, w_up[0].T, w_down[0]

        def gather(piece):
            return lax.all_gather(piece[None], "ep", axis=0, tiled=True)

        def swap(mine):
            far = lax.ppermute(mine, "dp", [(0, 1), (1, 0)])
            return far, lax.ppermute(far, "ep", partner_pairs)

        def same_core(own):
            return lax.dynamic_index_in_dim(own.reshape(chips, 2, *own.shape[1:]), core, 1, keepdims=False)

        half_rows = [lax.dynamic_slice_in_dim(w, side * ff_half, ff_half, 0) for w in (gate_rows, up_rows)]
        gu_own = gather(jnp.concatenate(half_rows, axis=0))
        down_own = gather(lax.dynamic_slice_in_dim(down_rows, side * col_half, col_half, 1))
        gate_rest = gather(gate_rows[ff_split:])
        up_rest = gather(up_rows[ff_split:])
        cut_rest = down_rows[:, col_split:]
        down_rest = gather(cut_rest)

        gu_mine = same_core(gu_own)
        gu_far, gu_other = swap(gu_mine)
        down_mine = same_core(down_own)
        down_wide, down_slim = down_mine[:, :, :wide], down_mine[:, :, wide:]
        down_wide = swap(down_wide)
        down_slim = swap(down_slim)

        normed = layer_norm(hidden, ln_gamma, ln_beta)
        position = copy_slots(choice, experts)
        flat_slot = jnp.where(position < capacity, choice * capacity + position, slot_count)
        token_ids = jnp.broadcast_to(jnp.arange(tokens, dtype=jnp.int32)[:, None], (tokens, 2))
        source_row = jnp.zeros((slot_count,), jnp.int32).at[flat_slot.reshape(-1)].set(token_ids.reshape(-1), mode="drop")
        rows = jnp.take(normed, source_row, axis=0, mode="clip").reshape(experts, capacity, row_width)

        gates = sparse_gates(normed, w_router, choice, mask_first, mask_second)
        gates = [jnp.where(position[:, j] < capacity, gates[j], 0.0) for j in range(2)]
        pick_slot = choice * capacity + jnp.minimum(position, capacity - 1)
        picks = [pick_slot[:, j] for j in range(2)]
        rows, gates, picks = lax.optimization_barrier((rows, gates, picks))

        by_core = rows.reshape(chips, 2, capacity, row_width)
        rows_mine = lax.dynamic_index_in_dim(by_core, core, 1, keepdims=False)
        rows_other = lax.dynamic_index_in_dim(by_core, 1 - core, 1, keepdims=False)

        def project(weight, rows=rows):
            return jnp.einsum("erd,efd->erf", rows, weight, preferred_element_type=jnp.float32)

        def activate(gate_proj, up_proj):
            return (jax.nn.silu(gate_proj) * up_proj).astype(jnp.bfloat16)

        def activate_both(both):
            return activate(both[:, :, :ff_half], both[:, :, ff_half:])

        act_own = activate_both(project(gu_own))
        act_mine = activate_both(project(gu_far, rows_mine))
        act_other = activate_both(project(gu_other, rows_other))
        even, odd = jnp.where(first_core, act_mine, act_other), jnp.where(first_core, act_other, act_mine)
        act_far = jnp.concatenate([even, odd], axis=1).reshape(act_own.shape)
        act_rest = activate(project(gate_rest), project(up_rest))
        act = jnp.concatenate([jnp.where(on_left, act_own, act_far), jnp.where(on_left, act_far, act_own), act_rest], axis=2)

        def place(prev, weights, start, width, weight_col=0):
            where = jnp.stack([jnp.asarray(start, jnp.int32), core.astype(jnp.int32)])
            return mix_columns(where, picks, gates, act, hidden, weights, prev, width, weight_col)

        own_start, far_start = side * col_half, (1 - side) * col_half
        slim, rest = col_half - wide, row_width - col_split - wide
        out = place(None, (down_own,), own_start, wide)
        out = place(out, (down_own,), own_start + wide, slim, wide)
        out = place(out, down_wide, far_start, wide)
        out = place(out, down_slim, far_start + wide, slim)
        out = place(out, (down_rest,), col_split, wide)
        return place(out, (down_rest,), col_split + wide, rest, wide)

    return jax.shard_map(device_step, mesh=mesh,
                         in_specs=(rows_spec, P(), P(), P(), P("ep"), P("ep"), P("ep"), rows_spec, rows_spec, rows_spec),
                         out_specs=rows_spec, check_vma=False)
```
